16 devices in a mesh: replica: 2 (over z), fsdp: 8 (over y, x, core).
Axes of the slice: x: 2, y: 2, z: 2, core: 2. Of those that a mesh axis runs over, the one named last changes fastest.
Arguments:
- block_in: bfloat16 [1, 32768, 2048], P(None, ('replica', 'fsdp'))
- grad_out: bfloat16 [32768, 2048], P(('replica', 'fsdp'))
- w_up: bfloat16 [1, 2048, 5632], P(None, 'fsdp')
- w_lin: bfloat16 [1, 2048, 5632], P(None, 'fsdp')
- w_down: bfloat16 [1, 5632, 2048], P(None, 'fsdp')
Outputs:
- output 1: float32 [1, 2048, 5632], P(None, 'fsdp')
- output 2: float32 [1, 2048, 5632], P(None, 'fsdp')
- output 3: float32 [1, 5632, 2048], P(None, 'fsdp')
- output 4: bfloat16 [32768, 2048], P(('replica', 'fsdp'))
All inputs are finite; a program needn't handle non-finite values.
Results may differ from the reference program's by a relative error of at most 0.001.
Values are sent between devices in bfloat16 or wider.
A program may use at most 1 GiB of HBM per device.

```python
import jax
import jax.numpy as jnp
from jax import lax

D = 2048
FF = 5632
LAYERS = 1
TOK_DEV = 2048
REPLICA = 2
FSDP = 8
TOKENS = TOK_DEV * REPLICA * FSDP
NUM_BLOCKS = REPLICA * FSDP
NORM_EPS = 1e-5


def setup_inputs(seed: int = 0) -> dict:
    key_list = jax.random.split(jax.random.key(seed), 5)
    block_in = jax.random.normal(key_list[0], (LAYERS, TOKENS, D), jnp.float32).astype(jnp.bfloat16)
    grad_out = jax.random.normal(key_list[1], (TOKENS, D), jnp.float32).astype(jnp.bfloat16)
    w_up = (jax.random.normal(key_list[2], (LAYERS, D, FF), jnp.float32) * D ** -0.5).astype(jnp.bfloat16)
    w_lin = (jax.random.normal(key_list[3], (LAYERS, D, FF), jnp.float32) * D ** -0.5).astype(jnp.bfloat16)
    w_down = (jax.random.normal(key_list[4], (LAYERS, FF, D), jnp.float32) * (0.5 * FF ** -0.5)).astype(jnp.bfloat16)
    return {'block_in': block_in, 'grad_out': grad_out, 'w_up': w_up, 'w_lin': w_lin, 'w_down': w_down}


def layer_grad(h_in, grad_acc, up_w, lin_w, down_w):
    h_f32 = h_in.astype(jnp.float32)
    inv_rms = lax.rsqrt(jnp.mean(h_f32 * h_f32, axis=-1, keepdims=True) + NORM_EPS)
    normed = h_f32 * inv_rms
    normed_b = normed.astype(jnp.bfloat16)
    pre_up = jnp.dot(normed_b, up_w, preferred_element_type=jnp.float32)
    pre_lin = jnp.dot(normed_b, lin_w, preferred_element_type=jnp.float32)
    up_sig = jax.nn.sigmoid(pre_up)
    up_act = pre_up * up_sig
    act_b = (up_act * pre_lin).astype(jnp.bfloat16)
    grad_b = grad_acc.astype(jnp.bfloat16)
    d_act = jnp.dot(grad_b, down_w.T, preferred_element_type=jnp.float32)
    d_up = (d_act * pre_lin * up_sig * (1.0 + pre_up * (1.0 - up_sig))).astype(jnp.bfloat16)
    d_lin = (d_act * up_act).astype(jnp.bfloat16)
    g_down = jnp.dot(act_b.T, grad_b, preferred_element_type=jnp.float32)
    g_up = jnp.dot(normed_b.T, d_up, preferred_element_type=jnp.float32)
    g_lin = jnp.dot(normed_b.T, d_lin, preferred_element_type=jnp.float32)
    d_norm = jnp.dot(d_up, up_w.T, preferred_element_type=jnp.float32) + jnp.dot(d_lin, lin_w.T, preferred_element_type=jnp.float32)
    d_h = inv_rms * (d_norm - normed * jnp.mean(d_norm * normed, axis=-1, keepdims=True))
    return grad_acc + d_h, g_up, g_lin, g_down


def reference(block_in, grad_out, w_up, w_lin, w_down):
    blocks_in = block_in.reshape(LAYERS, NUM_BLOCKS, TOK_DEV, D).transpose(1, 0, 2, 3)
    blocks_grad = grad_out.reshape(NUM_BLOCKS, TOK_DEV, D)

    def block_step(grad_sums, block_xs):
        h_block, g_block = block_xs

        def layer_step(grad_acc, layer_xs):
            h_layer, up_w, lin_w, down_w = layer_xs
            new_grad, g_up, g_lin, g_down = layer_grad(h_layer, grad_acc, up_w, lin_w, down_w)
            return new_grad, (g_up, g_lin, g_down)

        final_grad, layer_grads = lax.scan(layer_step, g_block.astype(jnp.float32), (h_block, w_up, w_lin, w_down), reverse=True)
        new_sums = tuple(old_part + new_part for old_part, new_part in zip(grad_sums, layer_grads))
        return new_sums, final_grad.astype(jnp.bfloat16)

    zero_sums = (jnp.zeros((LAYERS, D, FF), jnp.float32), jnp.zeros((LAYERS, D, FF), jnp.float32), jnp.zeros((LAYERS, FF, D), jnp.float32))
    grad_sums, grad_blocks = lax.scan(block_step, zero_sums, (blocks_in, blocks_grad))
    return grad_sums[0], grad_sums[1], grad_sums[2], grad_blocks.reshape(TOKENS, D)
```

```python
import jax
import jax.numpy as jnp
from jax import lax
from jax.sharding import PartitionSpec as P


NORM_EPS = 1e-5
F32 = jnp.float32
BF16 = jnp.bfloat16


def dot(a, b, da, db):
    return lax.dot_general(a, b, (((da,), (db,)), ((), ())), preferred_element_type=F32)


def after(value, *others):
    return lax.optimization_barrier((value, others))[0]


def pick(arr, idx, axis):
    return lax.dynamic_index_in_dim(arr, idx, axis, keepdims=False)


def solution(mesh):
    n_fsdp = mesh.shape['fsdp']
    tok_spec = P(('replica', 'fsdp'), None)
    act_spec = P(None, ('replica', 'fsdp'), None)
    weight_spec = P(None, 'fsdp', None)

    def swap(value, bit):
        return lax.ppermute(value, 'fsdp', [(i, i ^ bit) for i in range(n_fsdp)])

    def swap_z(value):
        return lax.ppermute(value, 'replica', [(0, 1), (1, 0)])

    def split_parity(w, blk):
        cols = [w[:, i * blk:(i + 1) * blk] for i in range(n_fsdp)]
        return jnp.concatenate(cols[0::2] + cols[1::2], axis=1)

    def local_step(block_in, grad_out, w_up, w_lin, w_down):
        layers, tok, dim = block_in.shape
        ff = w_up.shape[2]
        half = ff // 2
        rows = dim // n_fsdp
        ff_blk = ff // n_fsdp
        fi = lax.axis_index('fsdp').astype(jnp.uint32)
        core = (fi & 1).astype(jnp.int32)
        pos = (((fi >> 1) & 1).astype(jnp.int32), (fi >> 2).astype(jnp.int32))

        def slab1(g, first):
            g = g.reshape((2, 2) + g.shape[1:])
            return pick(g, 1 - pos[first], 1 - first)

        def send1(slab, first):
            return swap(slab, 2 << first)

        def add1(g, got, first):
            g = g.reshape((2, 2) + g.shape[1:])
            return pick(g, pos[first], 1 - first) + got

        def send2(part, first):
            return swap(pick(part, 1 - pos[1 - first], 0), 4 >> first)

        def add2(part, got, first):
            return pick(part, pos[1 - first], 0) + got

        def place_cols(totals):
            out = []
            for tot in totals:
                mine = lax.dynamic_slice_in_dim(tot, core * rows, rows, axis=0)
                other = lax.dynamic_slice_in_dim(tot, (1 - core) * rows, rows, axis=0)
                got = swap(other, 1)
                even = jnp.where(core == 0, mine, got)
                odd = jnp.where(core == 0, got, mine)
                for j in range(tot.shape[1] // ff_blk):
                    out += [even[:, j * ff_blk:(j + 1) * ff_blk], odd[:, j * ff_blk:(j + 1) * ff_blk]]
            return jnp.concatenate(out, axis=1)

        def take_cols(full):
            return lax.dynamic_slice_in_dim(full, core * half, half, axis=1)

        grad_acc = grad_out.astype(F32)
        up_list = []
        lin_list = []
        down_list = []
        for l in reversed(range(layers)):
            up_eo = split_parity(w_up[l], ff_blk)
            lin_eo = split_parity(after(w_lin[l], up_eo), ff_blk)
            lin_w = take_cols(lax.all_gather(lin_eo, 'fsdp', axis=0, tiled=True))
            up_w = take_cols(lax.all_gather(up_eo, 'fsdp', axis=0, tiled=True))
            down_w = lax.all_gather(after(w_down[l], lin_eo), 'fsdp', axis=0, tiled=True)
            down_w = pick(down_w.reshape(n_fsdp // 2, 2, ff_blk, dim), core, 1).reshape(half, dim)
            h_f32 = block_in[l].astype(F32)
            inv_rms = lax.rsqrt(jnp.mean(h_f32 * h_f32, axis=-1, keepdims=True) + NORM_EPS)
            normed = h_f32 * inv_rms
            n_own = normed.astype(BF16)
            gb_own = grad_acc.astype(BF16)
            n = jnp.concatenate([n_own, swap(n_own, 1)], axis=0)
            gb = jnp.concatenate([gb_own, swap(gb_own, 1)], axis=0)

            pre_lin = dot(n, lin_w, 1, 0)
            pre_up = dot(n, up_w, 1, 0)
            up_sig = jax.nn.sigmoid(pre_up)
            act_b = (pre_up * up_sig * pre_lin).astype(BF16)
            act_b, pre_up, pre_lin = lax.optimization_barrier((act_b, pre_up, pre_lin))

            hd = dim // 2
            down = [dot(act_b, gb[:, j * hd:(j + 1) * hd], 0, 0).reshape(4, ff_blk, hd) for j in range(2)]
            down_slab = [slab1(g, j) for j, g in enumerate(down)]
            down_got = [send1(g, j) for j, g in enumerate(down_slab)]

            up_sig = jax.nn.sigmoid(pre_up)
            up_act = pre_up * up_sig
            d_act = dot(after(gb, down_slab), down_w, 1, 1)
            d_up = (d_act * pre_lin * up_sig * (1.0 + pre_up * (1.0 - up_sig))).astype(BF16)
            d_lin = (d_act * up_act).astype(BF16)

            hc = half // 2
            up = [dot(n, d_up[:, j * hc:(j + 1) * hc], 0, 0).reshape(4, 2 * rows, hc) for j in range(2)]
            down_got = after(down_got, *up)
            down_part = [add1(down[j], down_got[j], j) for j in range(2)]
            down_got = [send2(down_part[j], j) for j in range(2)]
            up = after(up, down_part)
            up_slab = [slab1(up[j], j) for j in range(2)]
            up_got = [send1(up_slab[j], j) for j in range(2)]

            n_late, d_lin_late = after((n, d_lin), up_slab)
            lin = [dot(n_late, d_lin_late[:, j * hc:(j + 1) * hc], 0, 0).reshape(4, 2 * rows, hc) for j in range(2)]
            down_got = after(down_got, *lin)
            down_own = [add2(down_part[j], down_got[j], j) for j in range(2)]
            down_z = [swap_z(v) for v in down_own]

            d_up_late, d_lin_late = after((d_up, d_lin), down_own)
            d_norm_par = dot(d_up_late[tok:], up_w, 1, 1) + dot(d_lin_late[tok:], lin_w, 1, 1)
            d_norm_got = swap(d_norm_par, 1)
            up_got = after(up_got, d_norm_par)
            up_part = [add1(up[j], up_got[j], j) for j in range(2)]
            up_got = [send2(up_part[j], j) for j in range(2)]
            lin = after(lin, up_part)
            lin_slab = [slab1(lin[j], j) for j in range(2)]
            lin_got = [send1(lin_slab[j], j) for j in range(2)]

            d_up_late, d_lin_late = after((d_up_late, d_lin_late), lin_slab)
            d_norm = dot(d_up_late[:tok], up_w, 1, 1) + dot(d_lin_late[:tok], lin_w, 1, 1) + d_norm_got
            d_h = inv_rms * (d_norm - normed * jnp.mean(d_norm * normed, axis=-1, keepdims=True))
            grad_acc = grad_acc + d_h

            up_got = after(up_got, grad_acc)
            up_own = [add2(up_part[j], up_got[j], j) for j in range(2)]
            up_z = [swap_z(v) for v in up_own]
            lin_got, down_z = after((lin_got, down_z), up_own)
            down_list.insert(0, jnp.concatenate([a + b for a, b in zip(down_own, down_z)], axis=1))
            lin_part = [add1(lin[j], lin_got[j], j) for j in range(2)]
            lin_got = [send2(lin_part[j], j) for j in range(2)]
            up_z = after(up_z, lin_part)
            up_list.insert(0, place_cols([a + b for a, b in zip(up_own, up_z)]))
            lin_own = [add2(lin_part[j], lin_got[j], j) for j in range(2)]
            lin_list.insert(0, place_cols([v + swap_z(v) for v in lin_own]))
        return jnp.stack(up_list), jnp.stack(lin_list), jnp.stack(down_list), grad_acc.astype(BF16)

    return jax.shard_map(local_step, mesh=mesh, in_specs=(act_spec, tok_spec, weight_spec, weight_spec, weight_spec), out_specs=(weight_spec, weight_spec, weight_spec, tok_spec), check_vma=False)
```

```python
import jax
import jax.numpy as jnp
from jax import lax
from jax.sharding import PartitionSpec as P


NORM_EPS = 1e-5
F32 = jnp.float32
BF16 = jnp.bfloat16


def dot(a, b, da, db):
    return lax.dot_general(a, b, (((da,), (db,)), ((), ())), preferred_element_type=F32)


def after(value, *others):
    return lax.optimization_barrier((value, others))[0]


def pick(arr, idx, axis):
    return lax.dynamic_index_in_dim(arr, idx, axis, keepdims=False)


def solution(mesh):
    n_fsdp = mesh.shape['fsdp']
    tok_spec = P(('replica', 'fsdp'), None)
    act_spec = P(None, ('replica', 'fsdp'), None)
    weight_spec = P(None, 'fsdp', None)

    def swap(value, bit):
        return lax.ppermute(value, 'fsdp', [(i, i ^ bit) for i in range(n_fsdp)])

    def swap_z(value):
        return lax.ppermute(value, 'replica', [(0, 1), (1, 0)])

    def split_parity(w, blk):
        cols = [w[:, i * blk:(i + 1) * blk] for i in range(n_fsdp)]
        return jnp.concatenate(cols[0::2] + cols[1::2], axis=1)

    def local_step(block_in, grad_out, w_up, w_lin, w_down):
        layers, tok, dim = block_in.shape
        ff = w_up.shape[2]
        half = ff // 2
        rows = dim // n_fsdp
        ff_blk = ff // n_fsdp
        fi = lax.axis_index('fsdp').astype(jnp.uint32)
        core = (fi & 1).astype(jnp.int32)
        pos = (((fi >> 1) & 1).astype(jnp.int32), (fi >> 2).astype(jnp.int32))

        def slab1(g, first):
            g = g.reshape((2, 2) + g.shape[1:])
            return pick(g, 1 - pos[first], 1 - first)

        def send1(slab, first):
            return swap(slab, 2 << first)

        def add1(g, got, first):
            g = g.reshape((2, 2) + g.shape[1:])
            return pick(g, pos[first], 1 - first) + got

        def slab2(part, first):
            return pick(part, 1 - pos[1 - first], 0)

        def send2(slab, first):
            return swap(slab, 4 >> first)

        def add2(part, got, first):
            return pick(part, pos[1 - first], 0) + got

        def place_cols(halves):
            out = []
            for pieces in halves:
                evens, odds = [], []
                for tot in pieces:
                    mine = lax.dynamic_slice_in_dim(tot, core * rows, rows, axis=0)
                    other = lax.dynamic_slice_in_dim(tot, (1 - core) * rows, rows, axis=0)
                    got = swap(other, 1)
                    evens.append(jnp.where(core == 0, mine, got))
                    odds.append(jnp.where(core == 0, got, mine))
                even, odd = jnp.concatenate(evens, axis=1), jnp.concatenate(odds, axis=1)
                for j in range(even.shape[1] // ff_blk):
                    out += [even[:, j * ff_blk:(j + 1) * ff_blk], odd[:, j * ff_blk:(j + 1) * ff_blk]]
            return jnp.concatenate(out, axis=1)

        def take_cols(full):
            return lax.dynamic_slice_in_dim(full, core * (full.shape[1] // 2), full.shape[1] // 2, axis=1)

        grad_acc = grad_out.astype(F32)
        up_list = []
        lin_list = []
        down_list = []
        for l in reversed(range(layers)):
            up_eo = split_parity(w_up[l], ff_blk)
            lin_eo = split_parity(after(w_lin[l], up_eo), ff_blk)
            hc = half // 2
            up_w = take_cols(lax.all_gather(up_eo, 'fsdp', axis=0, tiled=True))
            lin_w = take_cols(lax.all_gather(lin_eo, 'fsdp', axis=0, tiled=True))
            down_w = lax.all_gather(after(w_down[l], lin_eo), 'fsdp', axis=0, tiled=True)
            down_w = pick(down_w.reshape(n_fsdp // 2, 2, ff_blk, dim), core, 1).reshape(2, hc, dim)
            h_f32 = block_in[l].astype(F32)
            inv_rms = lax.rsqrt(jnp.mean(h_f32 * h_f32, axis=-1, keepdims=True) + NORM_EPS)
            normed = h_f32 * inv_rms
            n_own = normed.astype(BF16)
            gb_own = grad_acc.astype(BF16)
            n = jnp.concatenate([n_own, swap(n_own, 1)], axis=0)
            gb = jnp.concatenate([gb_own, swap(gb_own, 1)], axis=0)

            pre_up = dot(n, up_w, 1, 0)
            pre_lin = dot(n, lin_w, 1, 0)
            act_b = (pre_up * jax.nn.sigmoid(pre_up) * pre_lin).astype(BF16)
            act_b, pre_up, pre_lin = lax.optimization_barrier((act_b, pre_up, pre_lin))

            hd = dim // 2
            down = [dot(act_b, gb[:, j * hd:(j + 1) * hd], 0, 0).reshape(4, ff_blk, hd) for j in range(2)]
            down_slab = [slab1(g, j) for j, g in enumerate(down)]
            down_got = [send1(g, j) for j, g in enumerate(down_slab)]

            def d_hidden(j, gb_j):
                u, v = pre_up[:, j * hc:(j + 1) * hc], pre_lin[:, j * hc:(j + 1) * hc]
                sig = jax.nn.sigmoid(u)
                d_act = dot(gb_j, down_w[j], 1, 1)
                d_u = (d_act * v * sig * (1.0 + u * (1.0 - sig))).astype(BF16)
                return d_u, (d_act * (u * sig)).astype(BF16)

            d_up0, d_lin0 = d_hidden(0, after(gb, down_slab))
            up0 = dot(n, d_up0, 0, 0).reshape(4, 2 * rows, hc)
            up_slab0 = slab1(up0, 0)
            up_got0 = send1(up_slab0, 0)
            down_got0 = after(down_got[0], up_slab0)
            down_part0 = add1(down[0], down_got0, 0)
            down_slab0 = slab2(down_part0, 0)
            down_got0 = send2(down_slab0, 0)
            d_up1, d_lin1 = d_hidden(1, after(gb, down_slab0))
            up1 = dot(n, d_up1, 0, 0).reshape(4, 2 * rows, hc)
            up_slab1 = slab1(up1, 1)
            up_got1 = send1(up_slab1, 1)
            down_got1 = after(down_got[1], up_slab1)
            down_part1 = add1(down[1], down_got1, 1)
            down_slab1 = slab2(down_part1, 1)
            down_got1 = send2(down_slab1, 1)
            edge = (hc // 256 + 1) * 128
            cut = [(0, edge), (edge, hc)]

            def lin_grad(n_late, d_l):
                return [dot(n_late, d_l[:, a:b], 0, 0).reshape(4, 2 * rows, b - a) for a, b in cut]

            lin0 = lin_grad(after(n, down_slab1), d_lin0)
            down_own0 = add2(down_part0, after(down_got0, lin0), 0)
            down_z0 = swap_z(down_own0)
            lin1 = lin_grad(after(n, down_own0), d_lin1)
            up_part0 = add1(up0, after(up_got0, lin1), 0)
            up_slab0 = slab2(up_part0, 0)
            up_got0 = send2(up_slab0, 0)
            lin0, lin1 = after((lin0, lin1), up_slab0)

            lin = list(zip(lin0, lin1))
            lin_slab = [slab1(lin[0][j], j) for j in range(2)]
            lin_got = [send1(lin_slab[j], j) for j in range(2)]
            down_own1 = add2(down_part1, after(down_got1, lin_slab), 1)
            down_z1 = swap_z(down_own1)

            d_up_late = after((d_up0, d_up1, d_lin0, d_lin1), down_own1)

            def d_norm_of(parts, sl):
                u0, u1, l0, l1 = [p[sl] for p in parts]
                return (dot(u0, up_w[:, :hc], 1, 1) + dot(u1, up_w[:, hc:], 1, 1)
                        + dot(l0, lin_w[:, :hc], 1, 1) + dot(l1, lin_w[:, hc:], 1, 1))

            d_norm_par = d_norm_of(d_up_late, slice(tok, 2 * tok))
            d_norm_got = swap(d_norm_par, 1)
            up_part1 = add1(up1, after(up_got1, d_norm_par), 1)
            up_slab1 = slab2(up_part1, 1)
            up_got1 = send2(up_slab1, 1)
            up_own0 = add2(up_part0, after(up_got0, up_slab1), 0)
            up_z0 = swap_z(up_own0)
            d_norm = d_norm_of(after(d_up_late, up_own0), slice(0, tok)) + d_norm_got
            up_own1 = add2(up_part1, after(up_got1, d_norm), 1)
            up_z1 = swap_z(up_own1)
            lin_part = [add1(lin[0][j], after(lin_got[j], up_own1), j) for j in range(2)]
            lin_slab = [slab2(lin_part[j], j) for j in range(2)]
            lin_got = [send2(lin_slab[j], j) for j in range(2)]
            lin_b_slab = [slab1(after(lin[1][j], lin_slab), j) for j in range(2)]
            lin_b_got = [send1(lin_b_slab[j], j) for j in range(2)]
            d_norm = after(d_norm, lin_b_slab)
            d_h = inv_rms * (d_norm - normed * jnp.mean(d_norm * normed, axis=-1, keepdims=True))
            grad_acc = grad_acc + d_h
            lin_own = [add2(lin_part[j], after(lin_got[j], lin_b_slab), j) for j in range(2)]
            lin_z = [swap_z(v) for v in lin_own]
            lin_b_part = [add1(lin[1][j], after(lin_b_got[j], lin_own), j) for j in range(2)]
            lin_b_slab = [slab2(lin_b_part[j], j) for j in range(2)]
            lin_b_got = [send2(lin_b_slab[j], j) for j in range(2)]
            lin_b_own = [add2(lin_b_part[j], lin_b_got[j], j) for j in range(2)]
            lin_b_z = [swap_z(v) for v in lin_b_own]
            down_z0, down_z1, up_z0, up_z1, lin_z = after((down_z0, down_z1, up_z0, up_z1, lin_z), lin_b_own)
            down_sum = [down_own0 + down_z0, down_own1 + down_z1]
            up_sum = [[up_own0 + up_z0], [up_own1 + up_z1]]
            lin_sum = [lin_own[j] + lin_z[j] for j in range(2)]
            down_list.insert(0, jnp.concatenate(down_sum, axis=1))
            up_list.insert(0, place_cols(up_sum))
            lin_b_z = after(lin_b_z, up_list[0], down_list[0])
            lin_list.insert(0, place_cols([[lin_sum[j], lin_b_own[j] + lin_b_z[j]] for j in range(2)]))
        return jnp.stack(up_list), jnp.stack(lin_list), jnp.stack(down_list), grad_acc.astype(BF16)

    return jax.shard_map(local_step, mesh=mesh, in_specs=(act_spec, tok_spec, weight_spec, weight_spec, weight_spec), out_specs=(weight_spec, weight_spec, weight_spec, tok_spec), check_vma=False)
```

```python
import jax
import jax.numpy as jnp
from jax import lax
from jax.sharding import PartitionSpec as P


NORM_EPS = 1e-5
F32 = jnp.float32
BF16 = jnp.bfloat16


def dot(a, b, da, db):
    return lax.dot_general(a, b, (((da,), (db,)), ((), ())), preferred_element_type=F32)


def after(value, *others):
    return lax.optimization_barrier((value, others))[0]


def pick(arr, idx, axis):
    return lax.dynamic_index_in_dim(arr, idx, axis, keepdims=False)


def solution(mesh):
    n_fsdp = mesh.shape['fsdp']
    tok_spec = P(('replica', 'fsdp'), None)
    act_spec = P(None, ('replica', 'fsdp'), None)
    weight_spec = P(None, 'fsdp', None)

    def swap(value, bit):
        return lax.ppermute(value, 'fsdp', [(i, i ^ bit) for i in range(n_fsdp)])

    def swap_z(value):
        return lax.ppermute(value, 'replica', [(0, 1), (1, 0)])

    def split_parity(w, blk):
        cols = [w[:, i * blk:(i + 1) * blk] for i in range(n_fsdp)]
        return jnp.concatenate(cols[0::2] + cols[1::2], axis=1)

    def local_step(block_in, grad_out, w_up, w_lin, w_down):
        layers, tok, dim = block_in.shape
        ff = w_up.shape[2]
        half = ff // 2
        rows = dim // n_fsdp
        ff_blk = ff // n_fsdp
        fi = lax.axis_index('fsdp').astype(jnp.uint32)
        core = (fi & 1).astype(jnp.int32)
        pos = (((fi >> 1) & 1).astype(jnp.int32), (fi >> 2).astype(jnp.int32))

        def slab1(g, first):
            g = g.reshape((2, 2) + g.shape[1:])
            return pick(g, 1 - pos[first], 1 - first)

        def send1(slab, first):
            return swap(slab, 2 << first)

        def add1(g, got, first):
            g = g.reshape((2, 2) + g.shape[1:])
            return pick(g, pos[first], 1 - first) + got

        def slab2(part, first):
            return pick(part, 1 - pos[1 - first], 0)

        def send2(slab, first):
            return swap(slab, 4 >> first)

        def add2(part, got, first):
            return pick(part, pos[1 - first], 0) + got

        def place_cols(halves):
            out = []
            for pieces in halves:
                evens, odds = [], []
                for tot in pieces:
                    mine = lax.dynamic_slice_in_dim(tot, core * rows, rows, axis=0)
                    other = lax.dynamic_slice_in_dim(tot, (1 - core) * rows, rows, axis=0)
                    got = swap(other, 1)
                    evens.append(jnp.where(core == 0, mine, got))
                    odds.append(jnp.where(core == 0, got, mine))
                even, odd = jnp.concatenate(evens, axis=1), jnp.concatenate(odds, axis=1)
                for j in range(even.shape[1] // ff_blk):
                    out += [even[:, j * ff_blk:(j + 1) * ff_blk], odd[:, j * ff_blk:(j + 1) * ff_blk]]
            return jnp.concatenate(out, axis=1)

        def take_cols(full):
            return lax.dynamic_slice_in_dim(full, core * (full.shape[1] // 2), full.shape[1] // 2, axis=1)

        grad_acc = grad_out.astype(F32)
        up_list = []
        lin_list = []
        down_list = []
        for l in reversed(range(layers)):
            up_eo = split_parity(w_up[l], ff_blk)
            lin_eo = split_parity(after(w_lin[l], up_eo), ff_blk)
            hc = half // 2
            up_w = take_cols(lax.all_gather(up_eo, 'fsdp', axis=0, tiled=True))
            lin_w = take_cols(lax.all_gather(lin_eo, 'fsdp', axis=0, tiled=True))
            down_w = lax.all_gather(after(w_down[l], lin_eo), 'fsdp', axis=0, tiled=True)
            down_w = pick(down_w.reshape(n_fsdp // 2, 2, ff_blk, dim), core, 1).reshape(2, hc, dim)
            h_f32 = block_in[l].astype(F32)
            inv_rms = lax.rsqrt(jnp.mean(h_f32 * h_f32, axis=-1, keepdims=True) + NORM_EPS)
            normed = h_f32 * inv_rms
            n_own = normed.astype(BF16)
            gb_own = grad_acc.astype(BF16)
            n = jnp.concatenate([n_own, swap(n_own, 1)], axis=0)
            gb = jnp.concatenate([gb_own, swap(gb_own, 1)], axis=0)

            pre_up = dot(n, up_w, 1, 0)
            pre_lin = dot(n, lin_w, 1, 0)
            act_b = (pre_up * jax.nn.sigmoid(pre_up) * pre_lin).astype(BF16)
            act_b, pre_up, pre_lin = lax.optimization_barrier((act_b, pre_up, pre_lin))

            hd = dim // 2
            down = [dot(act_b, gb[:, j * hd:(j + 1) * hd], 0, 0).reshape(4, ff_blk, hd) for j in range(2)]
            down_slab = [slab1(g, j) for j, g in enumerate(down)]
            down_got = [send1(g, j) for j, g in enumerate(down_slab)]

            def d_hidden(j, gb_j):
                u, v = pre_up[:, j * hc:(j + 1) * hc], pre_lin[:, j * hc:(j + 1) * hc]
                sig = jax.nn.sigmoid(u)
                d_act = dot(gb_j, down_w[j], 1, 1)
                d_u = (d_act * v * sig * (1.0 + u * (1.0 - sig))).astype(BF16)
                return d_u, (d_act * (u * sig)).astype(BF16)

            d_up0, d_lin0 = d_hidden(0, after(gb, down_slab))
            up0 = dot(n, d_up0, 0, 0).reshape(4, 2 * rows, hc)
            up_slab0 = slab1(up0, 0)
            up_got0 = send1(up_slab0, 0)
            down_got0 = after(down_got[0], up_slab0)
            down_part0 = add1(down[0], down_got0, 0)
            down_slab0 = slab2(down_part0, 0)
            down_got0 = send2(down_slab0, 0)
            d_up1, d_lin1 = d_hidden(1, after(gb, down_slab0))
            up1 = dot(n, d_up1, 0, 0).reshape(4, 2 * rows, hc)
            up_slab1 = slab1(up1, 1)
            up_got1 = send1(up_slab1, 1)
            down_got1 = after(down_got[1], up_slab1)
            down_part1 = add1(down[1], down_got1, 1)
            down_slab1 = slab2(down_part1, 1)
            down_got1 = send2(down_slab1, 1)
            edge = (hc // 256 + 1) * 128
            cut = [(0, edge), (edge, hc)]

            def lin_grad(n_late, d_l):
                return [dot(n_late, d_l[:, a:b], 0, 0).reshape(4, 2 * rows, b - a) for a, b in cut]

            lin0 = lin_grad(after(n, down_slab1), d_lin0)
            down_own0 = add2(down_part0, after(down_got0, lin0), 0)
            down_z0 = swap_z(down_own0)
            lin1 = lin_grad(after(n, down_own0), d_lin1)
            up_part0 = add1(up0, after(up_got0, lin1), 0)
            up_slab0 = slab2(up_part0, 0)
            up_got0 = send2(up_slab0, 0)
            lin0, lin1 = after((lin0, lin1), up_slab0)

            lin = list(zip(lin0, lin1))
            lin_slab = [slab1(lin[0][j], j) for j in range(2)]
            lin_got = [send1(lin_slab[j], j) for j in range(2)]
            down_own1 = add2(down_part1, after(down_got1, lin_slab), 1)
            down_z1 = swap_z(down_own1)

            up_part1 = add1(up1, after(up_got1, down_own1), 1)
            up_slab1 = slab2(up_part1, 1)
            up_got1 = send2(up_slab1, 1)

            def d_norm_term(i, sl, *earlier):
                d = after((d_up0, d_up1, d_lin0, d_lin1)[i], *earlier)[sl]
                return dot(d, (up_w, lin_w)[i // 2][:, (i % 2) * hc:(i % 2 + 1) * hc], 1, 1)

            theirs, ours = slice(tok, 2 * tok), slice(0, tok)
            d_norm_par = sum(d_norm_term(i, theirs, up_slab1) for i in range(1, 3)) + d_norm_term(0, theirs, up_slab1)
            up_own0 = add2(up_part0, after(up_got0, d_norm_par), 0)
            up_z0 = swap_z(up_own0)
            lin_b_slab = [slab1(after(lin[1][j], up_own0), j) for j in range(2)]
            lin_b_got = [send1(lin_b_slab[j], j) for j in range(2)]
            d_norm_par = after(d_norm_par, lin_b_slab) + d_norm_term(3, theirs, lin_b_slab)
            d_norm_got = swap(d_norm_par, 1)
            d_norm = d_norm_term(0, ours, d_norm_par)
            up_own1 = add2(up_part1, after(up_got1, d_norm), 1)
            up_z1 = swap_z(up_own1)
            lin_part = [add1(lin[0][j], after(lin_got[j], up_own1), j) for j in range(2)]
            lin_slab = [slab2(lin_part[j], j) for j in range(2)]
            lin_got = [send2(lin_slab[j], j) for j in range(2)]
            d_norm = d_norm + d_norm_term(1, ours, lin_slab) + d_norm_term(2, ours, lin_slab)
            lin_b_part = [add1(lin[1][j], after(lin_b_got[j], d_norm), j) for j in range(2)]
            lin_b_slab = [slab2(lin_b_part[j], j) for j in range(2)]
            lin_b_got = [send2(lin_b_slab[j], j) for j in range(2)]
            lin_own = [add2(lin_part[j], after(lin_got[j], lin_b_slab), j) for j in range(2)]
            lin_z = [swap_z(v) for v in lin_own]
            d_norm = after(d_norm, lin_own) + d_norm_term(3, ours, lin_own) + d_norm_got
            lin_b_got = after(lin_b_got, d_norm)
            d_h = inv_rms * (d_norm - normed * jnp.mean(d_norm * normed, axis=-1, keepdims=True))
            grad_acc = grad_acc + d_h
            lin_b_own = [add2(lin_b_part[j], lin_b_got[j], j) for j in range(2)]
            lin_b_z = [swap_z(v) for v in lin_b_own]
            down_z0, down_z1, up_z0, up_z1, lin_z = after((down_z0, down_z1, up_z0, up_z1, lin_z), lin_b_own)
            down_sum = [down_own0 + down_z0, down_own1 + down_z1]
            up_sum = [[up_own0 + up_z0], [up_own1 + up_z1]]
            lin_sum = [lin_own[j] + lin_z[j] for j in range(2)]
            down_list.insert(0, jnp.concatenate(down_sum, axis=1))
            up_list.insert(0, place_cols(up_sum))
            lin_b_z = after(lin_b_z, up_list[0], down_list[0])
            lin_list.insert(0, place_cols([[lin_sum[j], lin_b_own[j] + lin_b_z[j]] for j in range(2)]))
        return jnp.stack(up_list), jnp.stack(lin_list), jnp.stack(down_list), grad_acc.astype(BF16)

    return jax.shard_map(local_step, mesh=mesh, in_specs=(act_spec, tok_spec, weight_spec, weight_spec, weight_spec), out_specs=(weight_spec, weight_spec, weight_spec, tok_spec), check_vma=False)
```
